32 devices in a mesh: ga: 8 (over z, x), ta: 4 (over y, core).
Axes of the slice: x: 2, y: 2, z: 4, core: 2. Of those that a mesh axis runs over, the one named last changes fastest.
Arguments:
- density: bfloat16 [2, 6144, 16384], P(None, 'ga', 'ta'), may hold values from -6 to 6
- coulomb: float32 [6144], P('ga'), may hold values from 0.001275776 to 0.01275776
- row_block: int32 [1], replicated, may hold values from 0 to 67
Outputs:
- kernel: float32 [4, 4096, 2, 240], P('ta', 'ga')
The draws below stay inside these ranges and needn't reach their ends.
Inputs may be any that keep to these rules, and one draw needn't show every extreme that they name: The rows row_block * 240 to row_block * 240 + 239 lie among the 16384 transitions.
All inputs are finite; a program needn't handle non-finite values.
Results may differ from the reference program's by a relative error of at most 0.0025.
Values may be sent and summed in bfloat16 or wider, within the bound.
No kernel may reach another device: no remote copies, remote signals or barrier semaphores. Data moves between devices by JAX's collectives and lax.ppermute only.
A program may use at most 64 MiB of HBM per device.

```python
import math
import jax
import jax.numpy as jnp
from jax import lax

NG = 6144
NC = 16384
RB = 240
N_TA = 4


def shard_levels(key, dims, shards, least, high):
    gain, own = 1.0, jax.random.fold_in(key, 6)
    for position, shards_of in shards:
        steps = jnp.exp(jax.random.uniform(jax.random.fold_in(own, position), (shards_of,), jnp.float32, least / len(shards), high / len(shards)))
        gain = gain * jnp.repeat(steps, dims[position] // shards_of).reshape([-1 if axis == position else 1 for axis in range(len(dims))])
    return gain


def gaussian(stream_key, shape, scale, most, split=(), held_as=jnp.bfloat16):
    drawn = jax.random.normal(stream_key, shape, jnp.float32) * scale
    if len(split) > 0:
        drawn = shard_levels(stream_key, shape, split, -0.22, 0.18) * drawn
    return jnp.clip(drawn, min=-most, max=most).astype(held_as)


def setup_inputs(seed: int = 0) -> dict:
    key_list = jax.random.split(jax.random.key(seed), 4)
    density = gaussian(key_list[0], (2, NG, NC), 1.0, 6.0, ((1, 8), (2, 4)))
    coulomb = jnp.clip(jnp.exp(math.log(0.01275776) - 2.3025851 * jax.random.uniform(key_list[1], (NG,), jnp.float32) ** shard_levels(key_list[1], (NG,), ((0, 8),), -0.2, 0.2)), 0.001275776, 0.01275776)
    row_block = jax.random.randint(key_list[2], (1,), 0, NC // RB).astype(jnp.int32)
    return dict(density=density, coulomb=coulomb, row_block=row_block)


def stack_left(folded):
    real_part = folded[0]
    imag_part = folded[1]
    upper_half = jnp.concatenate([real_part, -imag_part], axis=1)
    lower_half = jnp.concatenate([imag_part, real_part], axis=1)
    return jnp.concatenate([upper_half, lower_half], axis=0)


def reference(density, coulomb, row_block):
    offset = (row_block[0] * RB).astype(jnp.int32)
    picked = lax.dynamic_slice_in_dim(density, offset, RB, 2)
    folded = (coulomb[None, :, None] * picked.astype(jnp.float32)).astype(jnp.bfloat16)
    stacked = stack_left(folded)
    flattened = density.reshape(2 * NG, NC)
    kernel = lax.dot_general(flattened, stacked, (((0,), (0,)), ((), ())), preferred_element_type=jnp.float32)
    return kernel.reshape(N_TA, NC // N_TA, 2, RB)
```

```python
import jax
import jax.numpy as jnp
from jax import lax
from jax.experimental import pallas as pl
from jax.experimental.pallas import tpu as pltpu
from jax.sharding import PartitionSpec as P

RB = 240
LANES = 128


def swap(value, axis, mask):
    size = lax.axis_size(axis)
    return lax.ppermute(value, axis, [(i, i ^ mask) for i in range(size)])


def pick_kernel(window, starts_ref, d0, d1, d2, coulomb_ref, out_ref):
    first = starts_ref[window]
    width = starts_ref[window + 1]
    row = lax.broadcasted_iota(jnp.int32, (RB, LANES), 0) + first
    lane = lax.broadcasted_iota(jnp.int32, (RB, LANES), 1)
    own = (row >= 0) & (row < width)
    weights = coulomb_ref[...]
    hots = []
    for w in range(window):
        base = starts_ref[w] * LANES
        fresh = starts_ref[window + 2 + w] == 1
        hots.append(jnp.where((lane + base == row) & own & fresh, 1.0, 0.0).astype(jnp.bfloat16))
    for p in range(2):
        total = None
        for hot, block in zip(hots, (d0, d1, d2)):
            term = lax.dot_general(
                hot, block[p], (((1,), (1,)), ((), ())), preferred_element_type=jnp.float32
            )
            total = term if total is None else total + term
        out_ref[p] = (weights * total).astype(jnp.bfloat16)


def pick(density, coulomb, row_block):
    _, local_g, width = density.shape
    first = row_block[0] * RB - lax.axis_index("ta") * width
    window = 3
    last = width // LANES - 1
    blocks = [first // LANES + w for w in range(window)]
    fresh = [((b >= 0) & (b <= last)).astype(jnp.int32) for b in blocks]
    blocks = [jnp.clip(b, 0, last) for b in blocks]
    starts = jnp.stack(blocks + [first, jnp.int32(width)] + fresh).astype(jnp.int32)
    block = lambda w: pl.BlockSpec((2, local_g, LANES), lambda i, s: (0, 0, s[w]))
    return pl.pallas_call(
        lambda *refs: pick_kernel(window, *refs),
        out_shape=jax.ShapeDtypeStruct((2, RB, local_g), jnp.bfloat16),
        grid_spec=pltpu.PrefetchScalarGridSpec(
            num_scalar_prefetch=1,
            grid=(1,),
            in_specs=[block(0), block(1), block(2), pl.BlockSpec((1, local_g), lambda i, s: (0, 0))],
            out_specs=pl.BlockSpec((2, RB, local_g), lambda i, s: (0, 0, 0)),
        ),
        name="pick",
    )(starts, density, density, density, coulomb.reshape(1, local_g))


def tile_kernel(order_ref, folded_ref, density_ref, out_ref, left):
    rows = folded_ref.shape[1]
    local_g = folded_ref.shape[2]

    @pl.when(pl.program_id(0) == 0)
    def _():
        left[:rows, :local_g] = folded_ref[0]
        left[:rows, local_g:] = folded_ref[1]
        left[rows:, :local_g] = -folded_ref[1]
        left[rows:, local_g:] = folded_ref[0]

    right = density_ref[...].reshape(2 * local_g, density_ref.shape[2])
    out_ref[0] = jnp.dot(left[...], right, preferred_element_type=jnp.float32).astype(out_ref.dtype)


def tiles(folded, density, order, own, dtype):
    rows, local_g = folded.shape[1:]
    count = order.shape[0]
    if own % LANES:
        real, imag = folded[0], folded[1]
        left = jnp.concatenate(
            [jnp.concatenate([real, imag], 1), jnp.concatenate([-imag, real], 1)], 0
        )
        right = density.reshape(2 * local_g, -1, own)
        right = jnp.take(right, order, axis=1)
        out = jnp.einsum("ik,krc->ric", left, right, preferred_element_type=jnp.float32)
        return out.astype(dtype)
    return pl.pallas_call(
        tile_kernel,
        out_shape=jax.ShapeDtypeStruct((count, 2 * rows, own), dtype),
        grid_spec=pltpu.PrefetchScalarGridSpec(
            num_scalar_prefetch=1,
            grid=(count,),
            in_specs=[
                pl.BlockSpec((2, rows, local_g), lambda r, s: (0, 0, 0)),
                pl.BlockSpec((2, local_g, own), lambda r, s: (0, 0, s[r])),
            ],
            out_specs=pl.BlockSpec((1, 2 * rows, own), lambda r, s: (r, 0, 0)),
            scratch_shapes=[pltpu.VMEM((2 * rows, 2 * local_g), jnp.bfloat16)],
        ),
        cost_estimate=pl.CostEstimate(
            flops=8 * rows * local_g * own * count,
            bytes_accessed=4 * local_g * own * count,
            transcendentals=0,
        ),
        name="tiles",
    )(order, folded, density)


def body(density, coulomb, row_block):
    devices = lax.axis_size("ga")
    own = density.shape[2] // devices
    me = lax.axis_index("ga")
    masks = ([1, 2, 6] + [1 << b for b in range(3, 30)])[: devices.bit_length() - 1]
    stages = len(masks)
    parts = stages
    rows = RB // parts

    picked = pick(density, coulomb, row_block)
    core = lax.axis_index("ta") % 2
    folded = []
    for p in range(parts):
        piece = picked[:, p * rows : (p + 1) * rows]
        piece = piece + swap(piece, "ta", 1)
        half = lax.dynamic_index_in_dim(piece, core, 0, keepdims=False)
        half = half + swap(half, "ta", 2)
        other = swap(half, "ta", 1)
        folded.append(
            jnp.where(core == 0, jnp.stack([half, other]), jnp.stack([other, half]))
        )

    kept, sent = [], []
    for p in range(parts):
        dims = masks[p:] + masks[:p]
        relative = []
        for r in range(devices):
            mask = 0
            for s in range(stages):
                if (r >> (stages - 1 - s)) & 1:
                    mask ^= dims[s]
            relative.append(mask)
        order = me ^ jnp.array(relative, jnp.int32)
        half = devices // 2
        sent.append(swap(tiles(folded[p], density, order[half:], own, jnp.bfloat16), "ga", dims[0]))
        kept.append((folded[p], order[:half]))
    kept = [tiles(f, density, o, own, jnp.float32) for f, o in kept]

    for s in range(stages):
        for p in range(parts):
            dims = masks[p:] + masks[:p]
            total = kept[p] + sent[p].astype(jnp.float32)
            half = total.shape[0] // 2
            if s + 1 < stages:
                sent[p] = swap(total[half:].astype(jnp.bfloat16), "ga", dims[s + 1])
                kept[p] = total[:half]
            else:
                kept[p] = total[0]
    out = jnp.concatenate([k.reshape(2, rows, own) for k in kept], axis=1)
    return out.transpose(2, 0, 1)[None]


def solution(mesh):
    in_specs = (P(None, "ga", "ta"), P("ga"), P())
    out_specs = P("ta", "ga", None, None)
    return jax.shard_map(body, mesh=mesh, in_specs=in_specs, out_specs=out_specs, check_vma=False)
```

```python
import functools

import jax
import jax.numpy as jnp
from jax import lax
from jax.experimental import pallas as pl
from jax.experimental.pallas import tpu as pltpu
from jax.sharding import PartitionSpec as P

RB = 240
LANES = 128


def swap(value, axis, mask):
    size = lax.axis_size(axis)
    return lax.ppermute(value, axis, [(i, i ^ mask) for i in range(size)])


def pick_kernel(first_ref, d0, d1, d2, coulomb_ref, *out_refs, width):
    first = first_ref[0]
    last = width // LANES - 1
    row = lax.broadcasted_iota(jnp.int32, (RB, LANES), 0) + first
    lane = lax.broadcasted_iota(jnp.int32, (RB, LANES), 1)
    total = None
    for w, block in enumerate((d0, d1, d2)):
        base = window_block(first, w)
        inside = (base >= 0) & (base <= last)
        start = jnp.where(inside, base * LANES, -4 * width)
        hot = jnp.where(lane + start == row, 1.0, 0.0).astype(jnp.bfloat16)
        term = lax.dot_general(
            hot, block[0], (((1,), (1,)), ((), ())), preferred_element_type=jnp.float32
        )
        total = term if total is None else total + term
    weighted = (coulomb_ref[...][None, :] * total).astype(jnp.bfloat16)
    rows = RB // len(out_refs)
    for k, out_ref in enumerate(out_refs):
        out_ref[0] = weighted[k * rows : (k + 1) * rows]


def window_block(first, w):
    return lax.shift_right_arithmetic(first, LANES.bit_length() - 1) + w


def pick(density, coulomb, row_block, parts):
    _, local_g, width = density.shape
    first = row_block * RB - lax.axis_index("ta") * width
    last = width // LANES - 1
    rows = RB // parts

    def block(w):
        return pl.BlockSpec(
            (1, local_g, LANES), lambda p, s: (p, 0, jnp.clip(window_block(s[0], w), 0, last))
        )

    return pl.pallas_call(
        functools.partial(pick_kernel, width=width),
        out_shape=[jax.ShapeDtypeStruct((2, rows, local_g), jnp.bfloat16)] * parts,
        grid_spec=pltpu.PrefetchScalarGridSpec(
            num_scalar_prefetch=1,
            grid=(2,),
            in_specs=[block(0), block(1), block(2), pl.BlockSpec((local_g,), lambda p, s: (0,))],
            out_specs=[pl.BlockSpec((1, rows, local_g), lambda p, s: (p, 0, 0))] * parts,
        ),
        name="pick",
    )(first, density, density, density, coulomb)


def near_kernel(order_ref, core_ref, *refs, parts):
    halves, others = refs[:parts], refs[parts : 2 * parts]
    density_ref = refs[2 * parts]
    left = refs[2 * parts + 1]
    outs = refs[2 * parts + 2 :]
    rows, local_g = halves[0].shape

    @pl.when(pl.program_id(0) == 0)
    def _():
        def fill(real_refs, imag_refs):
            for k in range(parts):
                at, mid, end = 2 * k * rows, (2 * k + 1) * rows, (2 * k + 2) * rows
                left[at:mid, :local_g] = real_refs[k][...]
                left[at:mid, local_g:] = imag_refs[k][...]
                left[mid:end, :local_g] = -imag_refs[k][...]
                left[mid:end, local_g:] = real_refs[k][...]

        pl.when(core_ref[0] == 0)(lambda: fill(halves, others))
        pl.when(core_ref[0] != 0)(lambda: fill(others, halves))

    split_tile(left, density_ref, outs, near_roles(parts), 2 * rows)


def far_kernel(order_ref, left, density_ref, *outs, parts):
    split_tile(left, density_ref, outs, far_roles(parts), left.shape[0] // parts)


NEAR = ((1, 1, 1), (1, 1, 0), (1, 0, 1), (0, 1, 1))
FAR = ((1, 0, 0), (0, 1, 0), (0, 0, 1), (0, 0, 0))


def near_roles(parts):
    kinds = {(1, 1, 1): (0, 0), (1, 1, 0): (0, 1), (1, 0, 1): (1, 0), (0, 1, 1): (2, 0)}
    return [[kinds[chunk[k:] + chunk[:k]] for k in range(parts)] for chunk in NEAR]


def far_roles(parts):
    kinds = {(1, 0, 0): (0, 0), (0, 1, 0): (1, 0), (0, 0, 1): (2, 0), (0, 0, 0): (3, 0)}
    return [[kinds[chunk[k:] + chunk[:k]] for k in range(parts)] for chunk in FAR]


def split_tile(left, density_ref, outs, roles, rows):
    right = density_ref[...].reshape(left.shape[1], density_ref.shape[2])
    parts = len(roles[0])
    product = jnp.dot(left[...], right, preferred_element_type=jnp.float32)
    for step, role in enumerate(roles):

        @pl.when(pl.program_id(0) == step)
        def _(role=role):
            for k, (kind, slot) in enumerate(role):
                ref = outs[kind * parts + k]
                ref[slot] = product[k * rows : (k + 1) * rows].astype(ref.dtype)


def split_call(kernel, name, scalars, operands, density, own, chunks, shapes):
    local_g = density.shape[1]
    vmem = pl.BlockSpec(memory_space=pltpu.VMEM)
    return pl.pallas_call(
        kernel,
        out_shape=shapes,
        grid_spec=pltpu.PrefetchScalarGridSpec(
            num_scalar_prefetch=len(scalars),
            grid=(chunks,),
            in_specs=[vmem] * len(operands)
            + [pl.BlockSpec((2, local_g, own), lambda r, s, *_: (0, 0, s[r]))],
            out_specs=[vmem] * len(shapes),
        ),
        cost_estimate=pl.CostEstimate(
            flops=8 * RB * local_g * own * chunks,
            bytes_accessed=4 * local_g * own * chunks,
            transcendentals=0,
        ),
        name=name,
    )(*scalars, *operands, density)


def exchange(halves, others, core, density, own, masks):
    parts = len(masks)
    rows, local_g = halves[0].shape
    me = lax.axis_index("ga")

    def order(chunks):
        return me ^ jnp.array(
            [xor_of(masks, c) for c in chunks],
            jnp.int32,
        )

    def shape(count, dtype):
        return jax.ShapeDtypeStruct((count, 2 * rows, own), dtype)

    bf16, f32 = jnp.bfloat16, jnp.float32
    left, *near = split_call(
        functools.partial(near_kernel, parts=parts),
        "near",
        (order(NEAR), core),
        (*halves, *others),
        density,
        own,
        len(NEAR),
        [jax.ShapeDtypeStruct((2 * rows * parts, 2 * local_g), bf16)]
        + [shape(2, bf16)] * parts
        + [shape(1, bf16)] * parts
        + [shape(1, f32)] * parts,
    )
    first, second, high = (near[k * parts : (k + 1) * parts] for k in range(3))
    dims = [masks[p:] + masks[:p] for p in range(parts)]
    first = [swap(v, "ga", d[0]) for v, d in zip(first, dims)]
    second = [swap(v, "ga", d[0]) for v, d in zip(second, dims)]
    far = split_call(
        functools.partial(far_kernel, parts=parts),
        "far",
        (order(FAR),),
        (left,),
        density,
        own,
        len(FAR),
        [shape(1, bf16)] * parts + [shape(1, f32)] * (3 * parts),
    )
    third, low, last, mine = (far[k * parts : (k + 1) * parts] for k in range(4))
    third = [swap(v, "ga", d[0]) for v, d in zip(third, dims)]
    middle = []
    for p in range(parts):
        send = jnp.concatenate([high[p], low[p]]) + first[p].astype(f32)
        middle.append(swap(send.astype(bf16), "ga", dims[p][1]))
    tail = []
    for p in range(parts):
        send = last[p] + second[p].astype(f32) + middle[p][:1].astype(f32)
        tail.append(swap(send.astype(bf16), "ga", dims[p][2]))
    done = []
    for p in range(parts):
        total = mine[p] + third[p].astype(f32) + middle[p][1:].astype(f32)
        done.append((total + tail[p].astype(f32)).reshape(2, rows, own))
    return done


def xor_of(masks, bits):
    mask = 0
    for m, bit in zip(masks, bits):
        mask ^= m * bit
    return mask


def tile_kernel(order_ref, folded_ref, density_ref, out_ref, left):
    rows = folded_ref.shape[1]
    local_g = folded_ref.shape[2]

    @pl.when(pl.program_id(0) == 0)
    def _():
        left[:rows, :local_g] = folded_ref[0]
        left[:rows, local_g:] = folded_ref[1]
        left[rows:, :local_g] = -folded_ref[1]
        left[rows:, local_g:] = folded_ref[0]

    right = density_ref[...].reshape(2 * local_g, density_ref.shape[2])
    out_ref[0] = jnp.dot(left[...], right, preferred_element_type=jnp.float32).astype(out_ref.dtype)


def tiles(folded, density, order, own, dtype):
    rows, local_g = folded.shape[1:]
    count = order.shape[0]
    if own % LANES:
        real, imag = folded[0], folded[1]
        left = jnp.concatenate(
            [jnp.concatenate([real, imag], 1), jnp.concatenate([-imag, real], 1)], 0
        )
        right = density.reshape(2 * local_g, -1, own)
        right = jnp.take(right, order, axis=1)
        out = jnp.einsum("ik,krc->ric", left, right, preferred_element_type=jnp.float32)
        return out.astype(dtype)
    return pl.pallas_call(
        tile_kernel,
        out_shape=jax.ShapeDtypeStruct((count, 2 * rows, own), dtype),
        grid_spec=pltpu.PrefetchScalarGridSpec(
            num_scalar_prefetch=1,
            grid=(count,),
            in_specs=[
                pl.BlockSpec((2, rows, local_g), lambda r, s: (0, 0, 0)),
                pl.BlockSpec((2, local_g, own), lambda r, s: (0, 0, s[r])),
            ],
            out_specs=pl.BlockSpec((1, 2 * rows, own), lambda r, s: (r, 0, 0)),
            scratch_shapes=[pltpu.VMEM((2 * rows, 2 * local_g), jnp.bfloat16)],
        ),
        cost_estimate=pl.CostEstimate(
            flops=8 * rows * local_g * own * count,
            bytes_accessed=4 * local_g * own * count,
            transcendentals=0,
        ),
        name="tiles",
    )(order, folded, density)


def body(density, coulomb, row_block):
    devices = lax.axis_size("ga")
    own = density.shape[2] // devices
    me = lax.axis_index("ga")
    masks = ([1, 2, 6] + [1 << b for b in range(3, 30)])[: devices.bit_length() - 1]
    stages = len(masks)
    parts = stages
    rows = RB // parts

    picked = pick(density, coulomb, row_block, parts)
    core = lax.axis_index("ta") % 2
    halves, others = [], []
    for piece in picked:
        piece = piece + swap(piece, "ta", 1)
        half = lax.dynamic_index_in_dim(piece, core, 0, keepdims=False)
        halves.append(half + swap(half, "ta", 2))
        others.append(swap(halves[-1], "ta", 1))

    if stages == 3 and own % LANES == 0:
        done = exchange(halves, others, core.reshape(1), density, own, masks)
        return jnp.concatenate(done, axis=1).transpose(2, 0, 1)[None]

    folded = [
        jnp.where(core == 0, jnp.stack([half, other]), jnp.stack([other, half]))
        for half, other in zip(halves, others)
    ]
    kept, sent = [], []
    for p in range(parts):
        dims = masks[p:] + masks[:p]
        relative = []
        for r in range(devices):
            mask = 0
            for s in range(stages):
                if (r >> (stages - 1 - s)) & 1:
                    mask ^= dims[s]
            relative.append(mask)
        order = me ^ jnp.array(relative, jnp.int32)
        half = devices // 2
        sent.append(swap(tiles(folded[p], density, order[half:], own, jnp.bfloat16), "ga", dims[0]))
        kept.append((folded[p], order[:half]))
    kept = [tiles(f, density, o, own, jnp.float32) for f, o in kept]

    for s in range(stages):
        for p in range(parts):
            dims = masks[p:] + masks[:p]
            total = kept[p] + sent[p].astype(jnp.float32)
            half = total.shape[0] // 2
            if s + 1 < stages:
                sent[p] = swap(total[half:].astype(jnp.bfloat16), "ga", dims[s + 1])
                kept[p] = total[:half]
            else:
                kept[p] = total[0]
    out = jnp.concatenate([k.reshape(2, rows, own) for k in kept], axis=1)
    return out.transpose(2, 0, 1)[None]


def solution(mesh):
    in_specs = (P(None, "ga", "ta"), P("ga"), P())
    out_specs = P("ta", "ga", None, None)
    return jax.shard_map(body, mesh=mesh, in_specs=in_specs, out_specs=out_specs, check_vma=False)
```

```python
import functools

import jax
import jax.numpy as jnp
from jax import lax
from jax.experimental import pallas as pl
from jax.experimental.pallas import tpu as pltpu
from jax.sharding import PartitionSpec as P

RB = 240
LANES = 128
VMEM_LIMITS = {"pick": 52 << 20, "near": 48 << 20, "far": 44 << 20}


def swap(value, axis, mask):
    size = lax.axis_size(axis)
    return lax.ppermute(value, axis, [(i, i ^ mask) for i in range(size)])


def pick_kernel(first_ref, d0, d1, d2, coulomb_ref, *out_refs, width):
    first = first_ref[0]
    last = width // LANES - 1
    row = lax.broadcasted_iota(jnp.int32, (RB, LANES), 0) + first
    lane = lax.broadcasted_iota(jnp.int32, (RB, LANES), 1)
    total = None
    for w, block in enumerate((d0, d1, d2)):
        base = window_block(first, w)
        inside = (base >= 0) & (base <= last)
        start = jnp.where(inside, base * LANES, -4 * width)
        hot = jnp.where(lane + start == row, 1.0, 0.0).astype(jnp.bfloat16)
        term = lax.dot_general(
            hot, block[0], (((1,), (1,)), ((), ())), preferred_element_type=jnp.float32
        )
        total = term if total is None else total + term
    weighted = (coulomb_ref[...][None, :] * total).astype(jnp.bfloat16)
    rows = RB // len(out_refs)
    for k, out_ref in enumerate(out_refs):
        out_ref[pl.program_id(0)] = weighted[k * rows : (k + 1) * rows]


def window_block(first, w):
    return lax.shift_right_arithmetic(first, LANES.bit_length() - 1) + w


def pick(density, coulomb, row_block, parts):
    _, local_g, width = density.shape
    first = row_block * RB - lax.axis_index("ta") * width
    last = width // LANES - 1
    rows = RB // parts

    def block(w):
        return pl.BlockSpec(
            (1, local_g, LANES), lambda p, s: (p, 0, jnp.clip(window_block(s[0], w), 0, last))
        )

    return pl.pallas_call(
        functools.partial(pick_kernel, width=width),
        out_shape=[jax.ShapeDtypeStruct((2, rows, local_g), jnp.bfloat16)] * parts,
        grid_spec=pltpu.PrefetchScalarGridSpec(
            num_scalar_prefetch=1,
            grid=(2,),
            in_specs=[block(0), block(1), block(2), pl.BlockSpec((local_g,), lambda p, s: (0,))],
            out_specs=[pl.BlockSpec(memory_space=pltpu.VMEM)] * parts,
        ),
        compiler_params=pltpu.CompilerParams(vmem_limit_bytes=VMEM_LIMITS["pick"]),
        name="pick",
    )(first, density, density, density, coulomb)


def near_kernel(me_ref, core_ref, *refs, parts):
    halves, others = refs[:parts], refs[parts : 2 * parts]
    density_ref = refs[2 * parts]
    left = refs[2 * parts + 1]
    outs = refs[2 * parts + 2 :]
    rows, local_g = halves[0].shape

    @pl.when(pl.program_id(0) == 0)
    def _():
        def fill(real_refs, imag_refs):
            for k in range(parts):
                at, mid, end = 2 * k * rows, (2 * k + 1) * rows, (2 * k + 2) * rows
                left[at:mid, :local_g] = real_refs[k][...]
                left[at:mid, local_g:] = imag_refs[k][...]
                left[mid:end, :local_g] = -imag_refs[k][...]
                left[mid:end, local_g:] = real_refs[k][...]

        pl.when(core_ref[0] == 0)(lambda: fill(halves, others))
        pl.when(core_ref[0] != 0)(lambda: fill(others, halves))

    split_tile(left, density_ref, outs, near_roles(parts), 2 * rows)


def far_kernel(me_ref, left, *refs, parts):
    split_tile(left, refs[parts], refs[parts + 1 :], far_roles(parts), left.shape[0] // parts)


NEAR = ((1, 1, 1), (1, 1, 0), (1, 0, 1), (0, 1, 1))
FAR = ((1, 0, 0), (0, 1, 0), (0, 0, 1), (0, 0, 0))


def near_roles(parts):
    kinds = {(1, 1, 1): (0, 0), (1, 1, 0): (0, 1), (1, 0, 1): (0, 2), (0, 1, 1): (1, 0)}
    return [[kinds[chunk[k:] + chunk[:k]] for k in range(parts)] for chunk in NEAR]


def far_roles(parts):
    kinds = {(0, 1, 0): (0, 1), (1, 0, 0): (1, 0), (0, 0, 1): (2, 0), (0, 0, 0): (3, 0)}
    return [[kinds[chunk[k:] + chunk[:k]] for k in range(parts)] for chunk in FAR]


def split_tile(left, density_ref, outs, roles, rows):
    right = density_ref[...].reshape(left.shape[1], density_ref.shape[2])
    parts = len(roles[0])
    product = jnp.dot(left[...], right, preferred_element_type=jnp.float32)
    for step, role in enumerate(roles):

        @pl.when(pl.program_id(0) == step)
        def _(role=role):
            for k, (kind, slot) in enumerate(role):
                ref = outs[kind * parts + k]
                ref[slot] = product[k * rows : (k + 1) * rows].astype(ref.dtype)


def split_call(kernel, name, scalars, operands, density, own, chunks, shapes, aliases={}):
    local_g = density.shape[1]
    vmem = pl.BlockSpec(memory_space=pltpu.VMEM)

    def owner(r, me):
        mask = chunks[-1]
        for k, other in enumerate(chunks[:-1]):
            mask = jnp.where(r == k, other, mask)
        return me ^ mask

    return pl.pallas_call(
        kernel,
        out_shape=shapes,
        grid_spec=pltpu.PrefetchScalarGridSpec(
            num_scalar_prefetch=len(scalars),
            grid=(len(chunks),),
            in_specs=[vmem] * len(operands)
            + [pl.BlockSpec((2, local_g, own), lambda r, s, *_: (0, 0, owner(r, s[0])))],
            out_specs=[vmem] * len(shapes),
        ),
        input_output_aliases=aliases,
        compiler_params=pltpu.CompilerParams(vmem_limit_bytes=VMEM_LIMITS[name]),
        cost_estimate=pl.CostEstimate(
            flops=8 * RB * local_g * own * len(chunks),
            bytes_accessed=4 * local_g * own * len(chunks),
            transcendentals=0,
        ),
        name=name,
    )(*scalars, *operands, density)


def exchange(halves, others, core, density, own, masks):
    parts = len(masks)
    rows, local_g = halves[0].shape
    me = lax.axis_index("ga").reshape(1)

    def order(chunks):
        return [xor_of(masks, c) for c in chunks]

    def shape(count, dtype):
        return jax.ShapeDtypeStruct((count, 2 * rows, own), dtype)

    bf16, f32 = jnp.bfloat16, jnp.float32
    left, *near = split_call(
        functools.partial(near_kernel, parts=parts),
        "near",
        (me, core),
        (*halves, *others),
        density,
        own,
        order(NEAR),
        [jax.ShapeDtypeStruct((2 * rows * parts, 2 * local_g), bf16)]
        + [shape(3, bf16)] * parts
        + [shape(2, f32)] * parts,
    )
    first, pair = near[:parts], near[parts:]
    dims = [masks[p:] + masks[:p] for p in range(parts)]
    first = [swap(v, "ga", d[0]) for v, d in zip(first, dims)]
    far = split_call(
        functools.partial(far_kernel, parts=parts),
        "far",
        (me,),
        (left, *pair),
        density,
        own,
        order(FAR),
        [shape(2, f32)] * parts + [shape(1, bf16)] * parts + [shape(1, f32)] * (2 * parts),
        {2 + k: k for k in range(parts)},
    )
    pair, second, last, mine = (far[k * parts : (k + 1) * parts] for k in range(4))
    second = [swap(v, "ga", d[0]) for v, d in zip(second, dims)]
    middle = []
    for p in range(parts):
        send = pair[p] + first[p][:2].astype(f32)
        middle.append(swap(send.astype(bf16), "ga", dims[p][1]))
    tail = []
    for p in range(parts):
        send = last[p] + first[p][2:].astype(f32) + middle[p][:1].astype(f32)
        tail.append(swap(send.astype(bf16), "ga", dims[p][2]))
    done = []
    for p in range(parts):
        total = mine[p] + second[p].astype(f32) + middle[p][1:].astype(f32)
        done.append((total + tail[p].astype(f32)).reshape(2, rows, own))
    return done


def xor_of(masks, bits):
    mask = 0
    for m, bit in zip(masks, bits):
        mask ^= m * bit
    return mask


def tile_kernel(order_ref, folded_ref, density_ref, out_ref, left):
    rows = folded_ref.shape[1]
    local_g = folded_ref.shape[2]

    @pl.when(pl.program_id(0) == 0)
    def _():
        left[:rows, :local_g] = folded_ref[0]
        left[:rows, local_g:] = folded_ref[1]
        left[rows:, :local_g] = -folded_ref[1]
        left[rows:, local_g:] = folded_ref[0]

    right = density_ref[...].reshape(2 * local_g, density_ref.shape[2])
    out_ref[0] = jnp.dot(left[...], right, preferred_element_type=jnp.float32).astype(out_ref.dtype)


def tiles(folded, density, order, own, dtype):
    rows, local_g = folded.shape[1:]
    count = order.shape[0]
    if own % LANES:
        real, imag = folded[0], folded[1]
        left = jnp.concatenate(
            [jnp.concatenate([real, imag], 1), jnp.concatenate([-imag, real], 1)], 0
        )
        right = density.reshape(2 * local_g, -1, own)
        right = jnp.take(right, order, axis=1)
        out = jnp.einsum("ik,krc->ric", left, right, preferred_element_type=jnp.float32)
        return out.astype(dtype)
    return pl.pallas_call(
        tile_kernel,
        out_shape=jax.ShapeDtypeStruct((count, 2 * rows, own), dtype),
        grid_spec=pltpu.PrefetchScalarGridSpec(
            num_scalar_prefetch=1,
            grid=(count,),
            in_specs=[
                pl.BlockSpec((2, rows, local_g), lambda r, s: (0, 0, 0)),
                pl.BlockSpec((2, local_g, own), lambda r, s: (0, 0, s[r])),
            ],
            out_specs=pl.BlockSpec((1, 2 * rows, own), lambda r, s: (r, 0, 0)),
            scratch_shapes=[pltpu.VMEM((2 * rows, 2 * local_g), jnp.bfloat16)],
        ),
        cost_estimate=pl.CostEstimate(
            flops=8 * rows * local_g * own * count,
            bytes_accessed=4 * local_g * own * count,
            transcendentals=0,
        ),
        name="tiles",
    )(order, folded, density)


def body(density, coulomb, row_block):
    devices = lax.axis_size("ga")
    own = density.shape[2] // devices
    me = lax.axis_index("ga")
    masks = ([1, 2, 6] + [1 << b for b in range(3, 30)])[: devices.bit_length() - 1]
    stages = len(masks)
    parts = stages
    rows = RB // parts

    picked = pick(density, coulomb, row_block, parts)
    core = lax.axis_index("ta") % 2
    halves, others = [], []
    for piece in picked:
        piece = piece + swap(piece, "ta", 1)
        half = lax.dynamic_index_in_dim(piece, core, 0, keepdims=False)
        halves.append(half + swap(half, "ta", 2))
        others.append(swap(halves[-1], "ta", 1))

    if stages == 3 and own % LANES == 0:
        done = exchange(halves, others, core.reshape(1), density, own, masks)
        return jnp.concatenate(done, axis=1).transpose(2, 0, 1)[None]

    folded = [
        jnp.where(core == 0, jnp.stack([half, other]), jnp.stack([other, half]))
        for half, other in zip(halves, others)
    ]
    kept, sent = [], []
    for p in range(parts):
        dims = masks[p:] + masks[:p]
        relative = []
        for r in range(devices):
            mask = 0
            for s in range(stages):
                if (r >> (stages - 1 - s)) & 1:
                    mask ^= dims[s]
            relative.append(mask)
        order = me ^ jnp.array(relative, jnp.int32)
        half = devices // 2
        sent.append(swap(tiles(folded[p], density, order[half:], own, jnp.bfloat16), "ga", dims[0]))
        kept.append((folded[p], order[:half]))
    kept = [tiles(f, density, o, own, jnp.float32) for f, o in kept]

    for s in range(stages):
        for p in range(parts):
            dims = masks[p:] + masks[:p]
            total = kept[p] + sent[p].astype(jnp.float32)
            half = total.shape[0] // 2
            if s + 1 < stages:
                sent[p] = swap(total[half:].astype(jnp.bfloat16), "ga", dims[s + 1])
                kept[p] = total[:half]
            else:
                kept[p] = total[0]
    out = jnp.concatenate([k.reshape(2, rows, own) for k in kept], axis=1)
    return out.transpose(2, 0, 1)[None]


def solution(mesh):
    in_specs = (P(None, "ga", "ta"), P("ga"), P())
    out_specs = P("ta", "ga", None, None)
    return jax.shard_map(body, mesh=mesh, in_specs=in_specs, out_specs=out_specs, check_vma=False)
```

```python
import functools

import jax
import jax.numpy as jnp
from jax import lax
from jax.experimental import pallas as pl
from jax.experimental.pallas import tpu as pltpu
from jax.sharding import PartitionSpec as P

RB = 240
LANES = 128
VMEM_LIMITS = {"pick": 52 << 20, "near": 48 << 20, "far": 44 << 20}


def swap(value, axis, mask):
    size = lax.axis_size(axis)
    return lax.ppermute(value, axis, [(i, i ^ mask) for i in range(size)])


def pick_kernel(first_ref, d0, d1, d2, coulomb_ref, *out_refs, width):
    first = first_ref[0]
    last = width // LANES - 1
    row = lax.broadcasted_iota(jnp.int32, (RB, LANES), 0) + first
    lane = lax.broadcasted_iota(jnp.int32, (RB, LANES), 1)
    total = None
    for w, block in enumerate((d0, d1, d2)):
        base = window_block(first, w)
        inside = (base >= 0) & (base <= last)
        start = jnp.where(inside, base * LANES, -4 * width)
        hot = jnp.where(lane + start == row, 1.0, 0.0).astype(jnp.bfloat16)
        term = lax.dot_general(
            hot, block[0], (((1,), (1,)), ((), ())), preferred_element_type=jnp.float32
        )
        total = term if total is None else total + term
    weighted = (coulomb_ref[...][None, :] * total).astype(jnp.bfloat16)
    rows = RB // len(out_refs)
    for k, out_ref in enumerate(out_refs):
        out_ref[pl.program_id(0)] = weighted[k * rows : (k + 1) * rows]


def window_block(first, w):
    return lax.shift_right_arithmetic(first, LANES.bit_length() - 1) + w


def pick(density, coulomb, row_block, parts):
    _, local_g, width = density.shape
    first = row_block * RB - lax.axis_index("ta") * width
    last = width // LANES - 1
    rows = RB // parts

    def block(w):
        return pl.BlockSpec(
            (1, local_g, LANES), lambda p, s: (p, 0, jnp.clip(window_block(s[0], w), 0, last))
        )

    return pl.pallas_call(
        functools.partial(pick_kernel, width=width),
        out_shape=[jax.ShapeDtypeStruct((2, rows, local_g), jnp.bfloat16)] * parts,
        grid_spec=pltpu.PrefetchScalarGridSpec(
            num_scalar_prefetch=1,
            grid=(2,),
            in_specs=[block(0), block(1), block(2), pl.BlockSpec((local_g,), lambda p, s: (0,))],
            out_specs=[pl.BlockSpec(memory_space=pltpu.VMEM)] * parts,
        ),
        compiler_params=pltpu.CompilerParams(vmem_limit_bytes=VMEM_LIMITS["pick"]),
        name="pick",
    )(first, density, density, density, coulomb)


def near_kernel(me_ref, core_ref, *refs, parts):
    halves, others = refs[:parts], refs[parts : 2 * parts]
    density_ref = refs[2 * parts]
    left = refs[2 * parts + 1]
    outs = refs[2 * parts + 2 :]
    rows, local_g = halves[0].shape

    @pl.when(pl.program_id(0) == 0)
    def _():
        def fill(real_refs, imag_refs):
            for k in range(parts):
                at, mid, end = 2 * k * rows, (2 * k + 1) * rows, (2 * k + 2) * rows
                left[at:mid, :local_g] = real_refs[k][...]
                left[at:mid, local_g:] = imag_refs[k][...]
                left[mid:end, :local_g] = -imag_refs[k][...]
                left[mid:end, local_g:] = real_refs[k][...]

        pl.when(core_ref[0] == 0)(lambda: fill(halves, others))
        pl.when(core_ref[0] != 0)(lambda: fill(others, halves))

    split_tile(left, density_ref, outs, near_roles(parts), 2 * rows)


def far_kernel(me_ref, left, *refs, parts):
    split_tile(left, refs[parts], refs[parts + 1 :], far_roles(parts), left.shape[0] // parts)


NEAR = ((1, 1, 1), (1, 1, 0), (1, 0, 1), (0, 1, 1))
FAR = ((1, 0, 0), (0, 1, 0), (0, 0, 1), (0, 0, 0))


def near_roles(parts):
    kinds = {(1, 1, 1): (0, 0), (1, 1, 0): (0, 1), (1, 0, 1): (0, 2), (0, 1, 1): (1, 0)}
    return [[kinds[chunk[k:] + chunk[:k]] for k in range(parts)] for chunk in NEAR]


def far_roles(parts):
    kinds = {(0, 1, 0): (0, 1), (1, 0, 0): (1, 0), (0, 0, 1): (2, 0), (0, 0, 0): (3, 0)}
    return [[kinds[chunk[k:] + chunk[:k]] for k in range(parts)] for chunk in FAR]


def split_tile(left, density_ref, outs, roles, rows):
    right = density_ref[...].reshape(left.shape[1], density_ref.shape[2])
    parts = len(roles[0])
    product = jnp.dot(left[...], right, preferred_element_type=jnp.float32)
    for step, role in enumerate(roles):

        @pl.when(pl.program_id(0) == step)
        def _(role=role):
            for k, (kind, slot) in enumerate(role):
                ref = outs[kind * parts + k]
                ref[slot] = product[k * rows : (k + 1) * rows].astype(ref.dtype)


def split_call(kernel, name, scalars, operands, density, own, chunks, shapes, aliases={}):
    local_g = density.shape[1]
    vmem = pl.BlockSpec(memory_space=pltpu.VMEM)

    def owner(r, me):
        mask = chunks[-1]
        for k, other in enumerate(chunks[:-1]):
            mask = jnp.where(r == k, other, mask)
        return me ^ mask

    return pl.pallas_call(
        kernel,
        out_shape=shapes,
        grid_spec=pltpu.PrefetchScalarGridSpec(
            num_scalar_prefetch=len(scalars),
            grid=(len(chunks),),
            in_specs=[vmem] * len(operands)
            + [pl.BlockSpec((2, local_g, own), lambda r, s, *_: (0, 0, owner(r, s[0])))],
            out_specs=[vmem] * len(shapes),
        ),
        input_output_aliases=aliases,
        compiler_params=pltpu.CompilerParams(vmem_limit_bytes=VMEM_LIMITS[name]),
        cost_estimate=pl.CostEstimate(
            flops=8 * RB * local_g * own * len(chunks),
            bytes_accessed=4 * local_g * own * len(chunks),
            transcendentals=0,
        ),
        name=name,
    )(*scalars, *operands, density)


def exchange(halves, others, core, density, own, masks):
    parts = len(masks)
    rows, local_g = halves[0].shape
    me = lax.axis_index("ga").reshape(1)

    def order(chunks):
        return [xor_of(masks, c) for c in chunks]

    def shape(count, dtype):
        return jax.ShapeDtypeStruct((count, 2 * rows, own), dtype)

    bf16, f32 = jnp.bfloat16, jnp.float32
    left, *near = split_call(
        functools.partial(near_kernel, parts=parts),
        "near",
        (me, core),
        (*halves, *others),
        density,
        own,
        order(NEAR),
        [jax.ShapeDtypeStruct((2 * rows * parts, 2 * local_g), bf16)]
        + [shape(3, bf16)] * parts
        + [shape(2, f32)] * parts,
    )
    first, pair = near[:parts], near[parts:]
    dims = [masks[p:] + masks[:p] for p in range(parts)]
    first = [swap(v, "ga", d[0]) for v, d in zip(first, dims)]
    far = split_call(
        functools.partial(far_kernel, parts=parts),
        "far",
        (me,),
        (left, *pair),
        density,
        own,
        order(FAR),
        [shape(2, f32)] * parts + [shape(1, bf16)] * parts + [shape(1, f32)] * (2 * parts),
        {2 + k: k for k in range(parts)},
    )
    pair, second, last, mine = (far[k * parts : (k + 1) * parts] for k in range(4))
    middle = []
    second = list(second)
    for p in range(parts):
        send = (pair[p] + first[p][:2].astype(f32)).astype(bf16)
        after = (p + 1) % parts
        send, second[after] = lax.optimization_barrier((send, second[after]))
        middle.append(swap(send, "ga", dims[p][1]))
        second[after] = swap(second[after], "ga", dims[after][0])
    tail = []
    for p in range(parts):
        send = last[p] + first[p][2:].astype(f32) + middle[p][:1].astype(f32)
        tail.append(swap(send.astype(bf16), "ga", dims[p][2]))
    done = []
    for p in range(parts):
        total = mine[p] + second[p].astype(f32) + middle[p][1:].astype(f32)
        done.append((total + tail[p].astype(f32)).reshape(2, rows, own))
    return done


def xor_of(masks, bits):
    mask = 0
    for m, bit in zip(masks, bits):
        mask ^= m * bit
    return mask


def tile_kernel(order_ref, folded_ref, density_ref, out_ref, left):
    rows = folded_ref.shape[1]
    local_g = folded_ref.shape[2]

    @pl.when(pl.program_id(0) == 0)
    def _():
        left[:rows, :local_g] = folded_ref[0]
        left[:rows, local_g:] = folded_ref[1]
        left[rows:, :local_g] = -folded_ref[1]
        left[rows:, local_g:] = folded_ref[0]

    right = density_ref[...].reshape(2 * local_g, density_ref.shape[2])
    out_ref[0] = jnp.dot(left[...], right, preferred_element_type=jnp.float32).astype(out_ref.dtype)


def tiles(folded, density, order, own, dtype):
    rows, local_g = folded.shape[1:]
    count = order.shape[0]
    if own % LANES:
        real, imag = folded[0], folded[1]
        left = jnp.concatenate(
            [jnp.concatenate([real, imag], 1), jnp.concatenate([-imag, real], 1)], 0
        )
        right = density.reshape(2 * local_g, -1, own)
        right = jnp.take(right, order, axis=1)
        out = jnp.einsum("ik,krc->ric", left, right, preferred_element_type=jnp.float32)
        return out.astype(dtype)
    return pl.pallas_call(
        tile_kernel,
        out_shape=jax.ShapeDtypeStruct((count, 2 * rows, own), dtype),
        grid_spec=pltpu.PrefetchScalarGridSpec(
            num_scalar_prefetch=1,
            grid=(count,),
            in_specs=[
                pl.BlockSpec((2, rows, local_g), lambda r, s: (0, 0, 0)),
                pl.BlockSpec((2, local_g, own), lambda r, s: (0, 0, s[r])),
            ],
            out_specs=pl.BlockSpec((1, 2 * rows, own), lambda r, s: (r, 0, 0)),
            scratch_shapes=[pltpu.VMEM((2 * rows, 2 * local_g), jnp.bfloat16)],
        ),
        cost_estimate=pl.CostEstimate(
            flops=8 * rows * local_g * own * count,
            bytes_accessed=4 * local_g * own * count,
            transcendentals=0,
        ),
        name="tiles",
    )(order, folded, density)


def body(density, coulomb, row_block):
    devices = lax.axis_size("ga")
    own = density.shape[2] // devices
    me = lax.axis_index("ga")
    masks = ([1, 2, 6] + [1 << b for b in range(3, 30)])[: devices.bit_length() - 1]
    stages = len(masks)
    parts = stages
    rows = RB // parts

    picked = pick(density, coulomb, row_block, parts)
    core = lax.axis_index("ta") % 2
    halves, others = [], []
    for piece in picked:
        piece = piece + swap(piece, "ta", 1)
        half = lax.dynamic_index_in_dim(piece, core, 0, keepdims=False)
        halves.append(half + swap(half, "ta", 2))
        others.append(swap(halves[-1], "ta", 1))

    if stages == 3 and own % LANES == 0:
        done = exchange(halves, others, core.reshape(1), density, own, masks)
        return jnp.concatenate(done, axis=1).transpose(2, 0, 1)[None]

    folded = [
        jnp.where(core == 0, jnp.stack([half, other]), jnp.stack([other, half]))
        for half, other in zip(halves, others)
    ]
    kept, sent = [], []
    for p in range(parts):
        dims = masks[p:] + masks[:p]
        relative = []
        for r in range(devices):
            mask = 0
            for s in range(stages):
                if (r >> (stages - 1 - s)) & 1:
                    mask ^= dims[s]
            relative.append(mask)
        order = me ^ jnp.array(relative, jnp.int32)
        half = devices // 2
        sent.append(swap(tiles(folded[p], density, order[half:], own, jnp.bfloat16), "ga", dims[0]))
        kept.append((folded[p], order[:half]))
    kept = [tiles(f, density, o, own, jnp.float32) for f, o in kept]

    for s in range(stages):
        for p in range(parts):
            dims = masks[p:] + masks[:p]
            total = kept[p] + sent[p].astype(jnp.float32)
            half = total.shape[0] // 2
            if s + 1 < stages:
                sent[p] = swap(total[half:].astype(jnp.bfloat16), "ga", dims[s + 1])
                kept[p] = total[:half]
            else:
                kept[p] = total[0]
    out = jnp.concatenate([k.reshape(2, rows, own) for k in kept], axis=1)
    return out.transpose(2, 0, 1)[None]


def solution(mesh):
    in_specs = (P(None, "ga", "ta"), P("ga"), P())
    out_specs = P("ta", "ga", None, None)
    return jax.shard_map(body, mesh=mesh, in_specs=in_specs, out_specs=out_specs, check_vma=False)
```
